128 devices in a mesh: dp: 16 (over z, y), tp: 8 (over x, core).
Axes of the slice: x: 4, y: 4, z: 4, core: 2. Of those that a mesh axis runs over, the one named last changes fastest.
Arguments:
- hidden: bfloat16 [1024, 4096], P(('dp', 'tp'))
- w_unembed: bfloat16 [4096, 131072], P(('dp', 'tp'))
Outputs:
- output: bfloat16 [1024, 131072], P(None, ('dp', 'tp'))
All inputs are finite; a program needn't handle non-finite values.
Results may differ from the reference program's by a relative error of at most 0.001.
Values are sent between devices in bfloat16 or wider.
A program may use at most 1 GiB of HBM per device.

```python
import jax
import jax.numpy as jnp
from jax import lax

TOTAL_ROWS = 1024
MODEL_DIM = 4096
VOCAB_SIZE = 131072
NUM_SHARDS = 128


def setup_inputs(seed: int = 0) -> dict:
    key_hidden, key_weight = jax.random.split(jax.random.key(seed))
    hidden = jax.random.normal(key_hidden, (TOTAL_ROWS, MODEL_DIM), jnp.float32)
    weight = jax.random.normal(key_weight, (MODEL_DIM, VOCAB_SIZE), jnp.float32) * MODEL_DIM ** -0.5
    return {"hidden": hidden.astype(jnp.bfloat16), "w_unembed": weight.astype(jnp.bfloat16)}


def reference(hidden, w_unembed):
    block_rows = TOTAL_ROWS // NUM_SHARDS

    def row_block(hid_blk):
        return jnp.dot(hid_blk, w_unembed, preferred_element_type=jnp.float32).astype(jnp.bfloat16)

    logits = lax.map(row_block, hidden.reshape(NUM_SHARDS, block_rows, MODEL_DIM))
    return logits.reshape(TOTAL_ROWS, VOCAB_SIZE)
```

```python
import functools

import jax
import jax.numpy as jnp
from jax import lax
from jax.experimental import pallas as pl
from jax.experimental.pallas import tpu as pltpu
from jax.sharding import PartitionSpec as P

MESH = pl.DeviceIdType.MESH
Z, Y, X = 0, 1, 2


def _turn(v):
    return (v[2], v[0], v[1])


def _neg(v):
    return tuple(-t % 4 for t in v)


def _routes():
    routes = {}
    for v in [(a, b, c) for a in range(4) for b in range(4) for c in range(4)]:
        if v == (0, 0, 0):
            continue
        w, order = v, (Z, Y, X)
        for _ in range(3):
            for u in (w, _neg(w)):
                if u not in routes:
                    routes[u] = tuple(a for a in order if u[a])
            w, order = _turn(w), tuple((a + 1) % 3 for a in order)
    routes[(1, 1, 1)], routes[(2, 2, 2)], routes[(3, 3, 3)] = (Z, Y, X), (Y, X, Z), (X, Z, Y)
    return routes


def _orbits(offsets):
    seen, groups = set(), []
    for v in offsets:
        if v in seen:
            continue
        group, w = [], v
        for _ in range(3):
            for u in (w, _neg(w)):
                if u not in seen:
                    seen.add(u)
                    group.append(u)
            w = _turn(w)
        groups.append(group)
    return groups


ROUTES = _routes()
THREE = _orbits([v for v in ROUTES if len(ROUTES[v]) == 3])
TWO = _orbits([v for v in ROUTES if len(ROUTES[v]) == 2])
ONE = [v for v in ROUTES if len(ROUTES[v]) == 1]
THREE_FLAT = [v for g in THREE for v in g]
TWO_FLAT = [v for g in TWO for v in g]
FIRST = THREE_FLAT + TWO_FLAT
PORTIONS = (((X, Y, Z), 0, 1408), ((Y, Z, X), 1408, 1408), ((Z, X, Y), 2816, 1280))


def _kernel(hid_ref, w_ref, out_ref, hbuf, wbuf, st_a, st_b, acc, r_a, r_b, r_k, s_w, r_h, s_h, r_x, s_x, l_sem):
    dp, tp = lax.axis_index("dp"), lax.axis_index("tp")
    pos, core = (dp // 4, dp % 4, tp // 2), tp % 2

    def shift(v):
        return tuple((p + d) % 4 if d else p for p, d in zip(pos, v))

    def dev(p, c):
        return (p[Z] * 4 + p[Y], p[X] * 2 + c)

    def chip(p):
        return (p[Z] * 4 + p[Y]) * 4 + p[X]

    def unit(axis, d):
        return tuple(d if a == axis else 0 for a in range(3))

    def send(src, dst, ssem, rsem, to):
        pltpu.make_async_remote_copy(
            src_ref=src, dst_ref=dst, send_sem=ssem, recv_sem=rsem, device_id=to, device_id_type=MESH
        ).start()

    def wait(ref, sem):
        pltpu.make_async_copy(ref, ref, sem).wait()

    barrier = pltpu.get_barrier_semaphore()
    peers = [dev(pos, 1 - core)]
    for axis in (X, Y, Z):
        for d in (1, 3, 2):
            for c in (core, 1 - core):
                peers.append(dev(shift(unit(axis, d)), c))
    for peer in peers:
        pl.semaphore_signal(barrier, inc=1, device_id=peer, device_id_type=MESH)
    pl.semaphore_wait(barrier, len(peers))

    def rows(slot, n=1):
        return pl.ds(pl.multiple_of(slot * 8, 8), n * 8)

    def runs(free, owner):
        out = []
        for z in range(4) if Z in free else (owner[Z],):
            for y in range(4) if Y in free and not (Y in free and X in free) else (owner[Y],):
                if X in free and Y in free:
                    out.append((core * 64 + z * 16, 16))
                elif X in free:
                    out.append((core * 64 + (z * 4 + y) * 4, 4))
                else:
                    out.append((core * 64 + (z * 4 + y) * 4 + owner[X], 1))
        return out

    def halves(part, col, width):
        if len(part) == 1 and part[0][1] == 1:
            cut = (width // 2 + 127) // 128 * 128
            s = part[0][0]
            return [(s, 1, col, cut)], [(s, 1, col + cut, width - cut)]
        if len(part) == 1:
            s, n = part[0]
            return [(s, n // 2, col, width)], [(s + n // 2, n // 2, col, width)]
        m = len(part) // 2
        return [(s, n, col, width) for s, n in part[:m]], [(s, n, col, width) for s, n in part[m:]]

    def sem_h(p, phase, step, side):
        return r_h.at[((p * 3 + phase) * 2 + step) * 2 + side]

    def hidden_send(phase, step):
        for p, (order, col, width) in enumerate(PORTIONS):
            axis, free = order[phase], order[:phase]
            for side, d in enumerate((1, 3)):
                to = dev(shift(unit(axis, d)), core)
                if step == 0:
                    items = [(s, n, col, width) for s, n in runs(free, pos)]
                else:
                    items = halves(runs(free, shift(unit(axis, 4 - d))), col, width)[side]
                for s, n, c0, cw in items:
                    dst = hbuf.at[rows(s, n), pl.ds(c0, cw)]
                    src = hid_ref.at[:, pl.ds(c0, cw)] if phase == 0 and step == 0 else dst
                    send(src, dst, s_h.at[p], sem_h(p, phase, step, side), to)

    def hidden_wait(phase, step):
        for p, (order, col, width) in enumerate(PORTIONS):
            n = 4**phase
            for side in range(2):
                if step == 0:
                    ref = hbuf.at[pl.ds(0, n * 8), pl.ds(col, width)]
                elif phase == 0:
                    cut = (width // 2 + 127) // 128 * 128
                    ref = hbuf.at[pl.ds(0, 8), pl.ds(col, cut if side == 0 else width - cut)]
                else:
                    ref = hbuf.at[pl.ds(0, n * 4), pl.ds(col, width)]
                wait(ref, sem_h(p, phase, step, side))

    def columns(c, n):
        return pl.ds(pl.multiple_of(c * 1024, 1024), n * 1024)

    def first_hop(v):
        i = FIRST.index(v)
        to = shift(unit(ROUTES[v][0], v[ROUTES[v][0]]))
        send(w_ref.at[:, columns(chip(shift(v)) * 2, 2)], st_a.at[i], s_w.at[0], r_a.at[i], dev(to, core))

    def deliver(src_of, v, last):
        axis, d = last
        to = shift(unit(axis, d))
        origin = tuple((t - o) % 4 for t, o in zip(to, v))
        at = wbuf.at[pl.ds(pl.multiple_of((chip(origin) * 2 + core) * 32, 32), 32)]
        for c in range(2):
            send(src_of(c), at, s_w.at[2], r_k.at[v[Z] * 4 + v[Y]], dev(to, c))

    def second_hop(v):
        i = FIRST.index(v)
        wait(st_a.at[i], r_a.at[i])
        axis = ROUTES[v][1]
        if len(ROUTES[v]) == 2:
            deliver(lambda c: st_a.at[i, :, pl.ds(c * 1024, 1024)], v, (axis, v[axis]))
        else:
            j = THREE_FLAT.index(v)
            send(st_a.at[i], st_b.at[j], s_w.at[1], r_b.at[j], dev(shift(unit(axis, v[axis])), core))

    def third_hop(v):
        j = THREE_FLAT.index(v)
        wait(st_b.at[j], r_b.at[j])
        axis = ROUTES[v][2]
        deliver(lambda c: st_b.at[j, :, pl.ds(c * 1024, 1024)], v, (axis, v[axis]))

    me = chip(pos) * 2 + core
    mine = wbuf.at[pl.ds(pl.multiple_of(me * 32, 32), 32)]
    slot = hbuf.at[rows(core * 64 + chip(pos))]
    pltpu.make_async_copy(hid_ref, slot, l_sem).start()
    pltpu.make_async_copy(w_ref.at[:, columns(me, 1)], mine, r_k.at[0]).start()

    fill = [[v for v in g] for g in THREE]
    batches = [fill[0], fill[1], fill[2], fill[3], [v for g in fill[4:] for v in g]]
    n = 0
    for phase in range(3):
        for step in range(2):
            hidden_send(phase, step)
            if n < len(batches):
                for v in batches[n]:
                    first_hop(v)
            n += 1
            if phase == 0 and step == 0:
                wait(slot, l_sem)
            if phase == 2:
                for g in TWO[:2] if step == 0 else TWO[2:]:
                    for v in g:
                        first_hop(v)
            if (phase, step) != (2, 1):
                hidden_wait(phase, step)
    send(w_ref.at[:, columns(chip(pos) * 2 + 1 - core, 1)], mine, s_w.at[2], r_k.at[0], dev(pos, 1 - core))

    for v in THREE_FLAT:
        second_hop(v)
    hidden_wait(2, 1)
    for p, (_, col, width) in enumerate(PORTIONS):
        half = hbuf.at[pl.ds(pl.multiple_of(core * 512, 512), 512), pl.ds(col, width)]
        send(half, half, s_x.at[p], r_x.at[p], dev(pos, 1 - core))
    for v in TWO_FLAT:
        second_hop(v)
    for v in ONE:
        axis = ROUTES[v][0]
        deliver(lambda c: w_ref.at[:, columns(chip(shift(v)) * 2 + c, 1)], v, (axis, v[axis]))
    for v in sorted(THREE_FLAT):
        third_hop(v)

    for p, (_, col, width) in enumerate(PORTIONS):
        wait(hbuf.at[pl.ds(0, 512), pl.ds(col, width)], r_x.at[p])

    def product(dz, dy, first):
        wait(wbuf.at[pl.ds(0, 256)], r_k.at[dz * 4 + dy])
        k0 = pl.multiple_of((((pos[Z] - dz) % 4) * 4 + (pos[Y] - dy) % 4) * 256, 256)
        for t in range(4):
            cols = pl.ds(t * 256, 256)
            part = jnp.dot(hbuf[:, pl.ds(k0, 256)], wbuf[pl.ds(k0, 256), cols], preferred_element_type=jnp.float32)
            if first:
                acc[:, cols] = part
            else:
                acc[:, cols] += part

    product(0, 0, True)

    @pl.loop(1, 7)
    def _(i):
        near = i < 4
        product(jnp.where(near, i, 0), jnp.where(near, 0, i - 3), False)

    @pl.loop(0, 9)
    def _(i):
        product(1 + i // 3, 1 + i % 3, False)

    @pl.loop(0, 64)
    def _(i):
        top = acc[pl.ds(pl.multiple_of(i * 8, 8), 8), :]
        low = acc[pl.ds(pl.multiple_of(512 + i * 8, 8), 8), :]
        out_ref[pl.ds(pl.multiple_of(i * 16, 16), 16), :] = jnp.concatenate([top, low], axis=0).astype(jnp.bfloat16)

    wait(st_a, s_w.at[0])
    wait(st_b, s_w.at[1])
    wait(wbuf.at[pl.ds(0, 127 * 32)], s_w.at[2])
    for p, (_, col, width) in enumerate(PORTIONS):
        wait(hbuf.at[pl.ds(0, 63 * 8), pl.ds(col, width)], s_h.at[p])
        wait(hbuf.at[pl.ds(0, 512), pl.ds(col, width)], s_x.at[p])


def solution(mesh):
    def local_part(hid_blk, w_blk):
        dma = pltpu.SemaphoreType.DMA
        return pl.pallas_call(
            _kernel,
            out_shape=jax.ShapeDtypeStruct((1024, 1024), jnp.bfloat16),
            in_specs=[pl.BlockSpec(memory_space=pl.ANY)] * 2,
            out_specs=pl.BlockSpec(memory_space=pltpu.VMEM),
            scratch_shapes=[
                pltpu.VMEM((1024, 4096), jnp.bfloat16),
                pltpu.VMEM((4096, 1024), jnp.bfloat16),
                pltpu.VMEM((len(FIRST), 32, 2048), jnp.bfloat16),
                pltpu.VMEM((len(THREE_FLAT), 32, 2048), jnp.bfloat16),
                pltpu.VMEM((1024, 1024), jnp.float32),
                dma((len(FIRST),)),
                dma((len(THREE_FLAT),)),
                dma((16,)),
                dma((3,)),
                dma((36,)),
                dma((3,)),
                dma((3,)),
                dma((3,)),
                dma,
            ],
            compiler_params=pltpu.CompilerParams(
                collective_id=0, has_side_effects=True, vmem_limit_bytes=58 * 2**20
            ),
        )(hid_blk, w_blk)

    return jax.shard_map(
        local_part,
        mesh=mesh,
        in_specs=(P(("dp", "tp"), None), P(("dp", "tp"), None)),
        out_specs=P(None, ("dp", "tp")),
        check_vma=False,
    )
```

```python
import functools

import jax
import jax.numpy as jnp
from jax import lax
from jax.experimental import pallas as pl
from jax.experimental.pallas import tpu as pltpu
from jax.sharding import PartitionSpec as P

MESH = pl.DeviceIdType.MESH
Z, Y, X = 0, 1, 2


def _turn(v):
    return (v[2], v[0], v[1])


def _neg(v):
    return tuple(-t % 4 for t in v)


def _routes():
    routes = {}
    for v in [(a, b, c) for a in range(4) for b in range(4) for c in range(4)]:
        if v == (0, 0, 0):
            continue
        w, order = v, tuple(sorted((Z, Y, X), key=lambda a: v[a] != 2))
        for _ in range(3):
            for u in (w, _neg(w)):
                if u not in routes:
                    routes[u] = tuple(a for a in order if u[a])
            w, order = _turn(w), tuple((a + 1) % 3 for a in order)
    routes[(1, 1, 1)], routes[(2, 2, 2)], routes[(3, 3, 3)] = (Z, Y, X), (Y, X, Z), (X, Z, Y)
    return routes


def _orbits(offsets):
    seen, groups = set(), []
    for v in offsets:
        if v in seen:
            continue
        group, w = [], v
        for _ in range(3):
            for u in (w, _neg(w)):
                if u not in seen:
                    seen.add(u)
                    group.append(u)
            w = _turn(w)
        groups.append(group)
    return groups


ROUTES = _routes()
THREE = _orbits([v for v in ROUTES if len(ROUTES[v]) == 3])
TWO = _orbits([v for v in ROUTES if len(ROUTES[v]) == 2])
ONE = [v for v in ROUTES if len(ROUTES[v]) == 1]
THREE_FLAT = [v for g in THREE for v in g]
TWO_FLAT = [v for g in TWO for v in g]
FIRST = THREE_FLAT + TWO_FLAT
GROUPS = {g[0]: g for g in THREE + TWO}
BATCHES = (
    GROUPS[1, 1, 2] + GROUPS[1, 1, 1] + GROUPS[2, 2, 2],
    GROUPS[1, 2, 2],
    GROUPS[1, 2, 3],
    GROUPS[1, 1, 3] + GROUPS[0, 1, 1],
    GROUPS[0, 1, 2],
    GROUPS[0, 1, 3] + GROUPS[0, 2, 1] + GROUPS[0, 2, 2],
)
PORTIONS = (((X, Y, Z), 0, 1152), ((Y, Z, X), 1152, 1536), ((Z, X, Y), 2688, 1408))


def _kernel(hid_ref, w_ref, out_ref, hbuf, wbuf, st_a, st_b, acc, r_a, r_b, r_k, s_w, r_h, s_h, r_x, s_x, l_sem):
    dp, tp = lax.axis_index("dp"), lax.axis_index("tp")
    pos, core = (dp // 4, dp % 4, tp // 2), tp % 2

    def shift(v):
        return tuple((p + d) % 4 if d else p for p, d in zip(pos, v))

    def dev(p, c):
        return (p[Z] * 4 + p[Y], p[X] * 2 + c)

    def chip(p):
        return (p[Z] * 4 + p[Y]) * 4 + p[X]

    def unit(axis, d):
        return tuple(d if a == axis else 0 for a in range(3))

    def send(src, dst, ssem, rsem, to):
        pltpu.make_async_remote_copy(
            src_ref=src, dst_ref=dst, send_sem=ssem, recv_sem=rsem, device_id=to, device_id_type=MESH
        ).start()

    def wait(ref, sem):
        pltpu.make_async_copy(ref, ref, sem).wait()

    barrier = pltpu.get_barrier_semaphore()
    peers = [dev(pos, 1 - core)]
    for axis in (X, Y, Z):
        for d in (1, 3, 2):
            for c in (core, 1 - core):
                peers.append(dev(shift(unit(axis, d)), c))
    for peer in peers:
        pl.semaphore_signal(barrier, inc=1, device_id=peer, device_id_type=MESH)
    pl.semaphore_wait(barrier, len(peers))

    def rows(slot, n=1):
        return pl.ds(pl.multiple_of(slot * 8, 8), n * 8)

    def runs(free, owner):
        out = []
        for z in range(4) if Z in free else (owner[Z],):
            for y in range(4) if Y in free and not (Y in free and X in free) else (owner[Y],):
                if X in free and Y in free:
                    out.append((core * 64 + z * 16, 16))
                elif X in free:
                    out.append((core * 64 + (z * 4 + y) * 4, 4))
                else:
                    out.append((core * 64 + (z * 4 + y) * 4 + owner[X], 1))
        return out

    def halves(part, col, width):
        if len(part) == 1 and part[0][1] == 1:
            cut = (width // 2 + 127) // 128 * 128
            s = part[0][0]
            return [(s, 1, col, cut)], [(s, 1, col + cut, width - cut)]
        if len(part) == 1:
            s, n = part[0]
            return [(s, n // 2, col, width)], [(s + n // 2, n // 2, col, width)]
        m = len(part) // 2
        return [(s, n, col, width) for s, n in part[:m]], [(s, n, col, width) for s, n in part[m:]]

    def sem_h(p, phase, step, side):
        return r_h.at[((p * 3 + phase) * 2 + step) * 2 + side]

    def hidden_send(phase, step):
        for p, (order, col, width) in enumerate(PORTIONS):
            axis, free = order[phase], order[:phase]
            for side, d in enumerate((1, 3)):
                to = dev(shift(unit(axis, d)), core)
                if step == 0:
                    items = [(s, n, col, width) for s, n in runs(free, pos)]
                else:
                    items = halves(runs(free, shift(unit(axis, 4 - d))), col, width)[side]
                for s, n, c0, cw in items:
                    dst = hbuf.at[rows(s, n), pl.ds(c0, cw)]
                    src = hid_ref.at[:, pl.ds(c0, cw)] if phase == 0 and step == 0 else dst
                    send(src, dst, s_h.at[p], sem_h(p, phase, step, side), to)

    def hidden_wait(phase, step):
        for p, (order, col, width) in enumerate(PORTIONS):
            n = 4**phase
            for side in range(2):
                if step == 0:
                    ref = hbuf.at[pl.ds(0, n * 8), pl.ds(col, width)]
                elif phase == 0:
                    cut = (width // 2 + 127) // 128 * 128
                    ref = hbuf.at[pl.ds(0, 8), pl.ds(col, cut if side == 0 else width - cut)]
                else:
                    ref = hbuf.at[pl.ds(0, n * 4), pl.ds(col, width)]
                wait(ref, sem_h(p, phase, step, side))

    def columns(c, n):
        return pl.ds(pl.multiple_of(c * 1024, 1024), n * 1024)

    def first_hop(v):
        i = FIRST.index(v)
        to = shift(unit(ROUTES[v][0], v[ROUTES[v][0]]))
        send(w_ref.at[:, columns(chip(shift(v)) * 2, 2)], st_a.at[i], s_w.at[0], r_a.at[i], dev(to, core))

    def deliver(src_of, v, last):
        axis, d = last
        to = shift(unit(axis, d))
        origin = tuple((t - o) % 4 for t, o in zip(to, v))
        at = wbuf.at[pl.ds(pl.multiple_of((chip(origin) * 2 + core) * 32, 32), 32)]
        for c in (1, 0) if sum(v) % 2 else (0, 1):
            send(src_of(c), at, s_w.at[2], r_k.at[v[Z] * 4 + v[Y]], dev(to, c))

    def second_hop(v):
        i = FIRST.index(v)
        wait(st_a.at[i], r_a.at[i])
        axis = ROUTES[v][1]
        if len(ROUTES[v]) == 2:
            deliver(lambda c: st_a.at[i, :, pl.ds(c * 1024, 1024)], v, (axis, v[axis]))
        else:
            j = THREE_FLAT.index(v)
            send(st_a.at[i], st_b.at[j], s_w.at[1], r_b.at[j], dev(shift(unit(axis, v[axis])), core))

    def third_hop(v):
        j = THREE_FLAT.index(v)
        wait(st_b.at[j], r_b.at[j])
        axis = ROUTES[v][2]
        deliver(lambda c: st_b.at[j, :, pl.ds(c * 1024, 1024)], v, (axis, v[axis]))

    me = chip(pos) * 2 + core
    mine = wbuf.at[pl.ds(pl.multiple_of(me * 32, 32), 32)]
    slot = hbuf.at[rows(core * 64 + chip(pos))]
    pltpu.make_async_copy(hid_ref, slot, l_sem).start()
    pltpu.make_async_copy(w_ref.at[:, columns(me, 1)], mine, r_k.at[0]).start()

    for n, batch in enumerate(BATCHES):
        phase, step = divmod(n, 2)
        hidden_send(phase, step)
        if n == 1:
            for v in ONE:
                axis = ROUTES[v][0]
                deliver(lambda c: w_ref.at[:, columns(chip(shift(v)) * 2 + c, 1)], v, (axis, v[axis]))
        for v in batch:
            first_hop(v)
        if n == 0:
            wait(slot, l_sem)
        if n < 5:
            hidden_wait(phase, step)
    send(w_ref.at[:, columns(chip(pos) * 2 + 1 - core, 1)], mine, s_w.at[2], r_k.at[0], dev(pos, 1 - core))

    for v in THREE_FLAT:
        second_hop(v)
    hidden_wait(2, 1)
    for p, (_, col, width) in enumerate(PORTIONS):
        half = hbuf.at[pl.ds(pl.multiple_of(core * 512, 512), 512), pl.ds(col, width)]
        send(half, half, s_x.at[p], r_x.at[p], dev(pos, 1 - core))
    for v in TWO_FLAT:
        second_hop(v)
    for v in sorted(THREE_FLAT):
        third_hop(v)

    for p, (_, col, width) in enumerate(PORTIONS):
        wait(hbuf.at[pl.ds(0, 512), pl.ds(col, width)], r_x.at[p])

    def product(dz, dy, first):
        wait(wbuf.at[pl.ds(0, 256)], r_k.at[dz * 4 + dy])
        k0 = pl.multiple_of((((pos[Z] - dz) % 4) * 4 + (pos[Y] - dy) % 4) * 256, 256)
        for t in range(4):
            cols = pl.ds(t * 256, 256)
            part = jnp.dot(hbuf[:, pl.ds(k0, 256)], wbuf[pl.ds(k0, 256), cols], preferred_element_type=jnp.float32)
            if first:
                acc[:, cols] = part
            else:
                acc[:, cols] += part

    product(0, 0, True)

    @pl.loop(1, 7)
    def _(i):
        near = i < 4
        product(jnp.where(near, i, 0), jnp.where(near, 0, i - 3), False)

    @pl.loop(0, 9)
    def _(i):
        product(1 + i // 3, 1 + i % 3, False)

    @pl.loop(0, 64)
    def _(i):
        top = acc[pl.ds(pl.multiple_of(i * 8, 8), 8), :]
        low = acc[pl.ds(pl.multiple_of(512 + i * 8, 8), 8), :]
        out_ref[pl.ds(pl.multiple_of(i * 16, 16), 16), :] = jnp.concatenate([top, low], axis=0).astype(jnp.bfloat16)

    wait(st_a, s_w.at[0])
    wait(st_b, s_w.at[1])
    wait(wbuf.at[pl.ds(0, 127 * 32)], s_w.at[2])
    for p, (_, col, width) in enumerate(PORTIONS):
        wait(hbuf.at[pl.ds(0, 63 * 8), pl.ds(col, width)], s_h.at[p])
        wait(hbuf.at[pl.ds(0, 512), pl.ds(col, width)], s_x.at[p])


def solution(mesh):
    def local_part(hid_blk, w_blk):
        dma = pltpu.SemaphoreType.DMA
        return pl.pallas_call(
            _kernel,
            out_shape=pltpu.VMEM((1024, 1024), jnp.bfloat16),
            in_specs=[pl.BlockSpec(memory_space=pl.ANY)] * 2,
            out_specs=pl.BlockSpec(memory_space=pltpu.VMEM),
            scratch_shapes=[
                pltpu.VMEM((1024, 4096), jnp.bfloat16),
                pltpu.VMEM((4096, 1024), jnp.bfloat16),
                pltpu.VMEM((len(FIRST), 32, 2048), jnp.bfloat16),
                pltpu.VMEM((len(THREE_FLAT), 32, 2048), jnp.bfloat16),
                pltpu.VMEM((1024, 1024), jnp.float32),
                dma((len(FIRST),)),
                dma((len(THREE_FLAT),)),
                dma((16,)),
                dma((3,)),
                dma((36,)),
                dma((3,)),
                dma((3,)),
                dma((3,)),
                dma,
            ],
            compiler_params=pltpu.CompilerParams(
                collective_id=0, has_side_effects=True, vmem_limit_bytes=58 * 2**20
            ),
        )(hid_blk, w_blk)

    return jax.shard_map(
        local_part,
        mesh=mesh,
        in_specs=(P(("dp", "tp"), None), P(("dp", "tp"), None)),
        out_specs=P(None, ("dp", "tp")),
        check_vma=False,
    )
```

```python
import functools

import jax
import jax.numpy as jnp
from jax import lax
from jax.experimental import pallas as pl
from jax.experimental.pallas import tpu as pltpu
from jax.sharding import PartitionSpec as P

MESH = pl.DeviceIdType.MESH
Z, Y, X = 0, 1, 2


def _turn(v):
    return (v[2], v[0], v[1])


def _neg(v):
    return tuple(-t % 4 for t in v)


def _last(v):
    z, y, x = v
    if sum(map(bool, v)) == 1:
        return next(a for a in range(3) if v[a])
    if x == 0:
        return Y if z == 2 or (y != 2 and z != y) else Z
    if z == 0 or y == 0:
        line, axis = (y, Y) if z == 0 else (z, Z)
        return axis if line != 2 and x in (2, line) else X
    if z == 2 and y == 2:
        return Y if x == 2 else X
    if z == 2:
        return Y if x in (2, y) else X
    if y == 2:
        return Z if x in (2, z) else X
    return Z if x == 2 else Y if x == z else X


def _route(v):
    last = _last(v)
    rest = [a for a in range(3) if v[a] and a != last]
    if len(rest) == 2:
        longer = [a for a in rest if v[a] == 2]
        if len(longer) == 1:
            first = longer[0]
        elif longer:
            first = X if X in rest else Z if v[X] == 1 else Y
        else:
            first = Z if last == Y else Y
        rest = [first] + [a for a in rest if a != first]
    return (*rest, last)


ALL = [(a, b, c) for a in range(4) for b in range(4) for c in range(4)][1:]
ROUTES = {v: _route(v) for v in ALL}
ONE = [v for v in ALL if len(ROUTES[v]) == 1]


def _lines(*lines):
    return [(*line, x) for line in lines for x in (1, 2, 3)]


G = dict(
    Q=_lines((2, 1), (2, 3), (1, 2), (3, 2)),
    T=_lines((2, 2)),
    P=_lines((1, 3), (3, 1)),
    R=_lines((1, 1), (3, 3)),
    A=_lines((0, 1), (0, 3)),
    B=_lines((0, 2)),
    C=_lines((2, 0)),
    D=_lines((1, 0), (3, 0)),
    E=[(a, b, 0) for a, b in ((2, 2), (2, 1), (2, 3), (1, 2), (3, 2), (1, 3), (3, 1), (1, 1), (3, 3))],
)
G["O"] = ONE
THREE_FLAT = G["T"] + G["Q"] + G["P"] + G["R"]
TWO_FLAT = G["A"] + G["D"] + G["B"] + G["C"] + G["E"]
FIRST = THREE_FLAT + TWO_FLAT


ORDER = [(0, 0), (0, 1), (0, 3), (1, 0), (3, 0), (0, 2), (2, 0), (2, 2), (1, 2), (3, 2), (2, 1), (2, 3), (1, 3), (3, 1), (1, 1), (3, 3)]
BATCHES = (
    G["Q"],
    G["O"] + G["T"],
    G["P"] + G["R"],
    G["A"] + G["B"] + G["C"],
    G["D"] + G["E"],
    [],
)
LATE = 2
PORTIONS = (((X, Y, Z), 0, 1152), ((Y, Z, X), 1152, 1536), ((Z, X, Y), 2688, 1408))


def _kernel(hid_ref, w_ref, acc, hbuf, wbuf, st_a, st_b, r_a, r_b, r_k, s_w, r_h, s_h, r_x, s_x, l_sem):
    dp, tp = lax.axis_index("dp"), lax.axis_index("tp")
    pos, core = (dp // 4, dp % 4, tp // 2), tp % 2

    def shift(v):
        return tuple((p + d) % 4 if d else p for p, d in zip(pos, v))

    def dev(p, c):
        return (p[Z] * 4 + p[Y], p[X] * 2 + c)

    def chip(p):
        return (p[Z] * 4 + p[Y]) * 4 + p[X]

    def unit(axis, d):
        return tuple(d if a == axis else 0 for a in range(3))

    def send(src, dst, ssem, rsem, to):
        pltpu.make_async_remote_copy(
            src_ref=src, dst_ref=dst, send_sem=ssem, recv_sem=rsem, device_id=to, device_id_type=MESH
        ).start()

    def wait(ref, sem):
        pltpu.make_async_copy(ref, ref, sem).wait()

    barrier = pltpu.get_barrier_semaphore()
    peers = [dev(pos, 1 - core)]
    for axis in (X, Y, Z):
        for d in (1, 3, 2):
            for c in (core, 1 - core):
                peers.append(dev(shift(unit(axis, d)), c))
    for peer in peers:
        pl.semaphore_signal(barrier, inc=1, device_id=peer, device_id_type=MESH)
    pl.semaphore_wait(barrier, len(peers))

    def rows(slot, n=1):
        return pl.ds(pl.multiple_of(slot * 8, 8), n * 8)

    def runs(free, owner):
        out = []
        for z in range(4) if Z in free else (owner[Z],):
            for y in range(4) if Y in free and not (Y in free and X in free) else (owner[Y],):
                if X in free and Y in free:
                    out.append((core * 64 + z * 16, 16))
                elif X in free:
                    out.append((core * 64 + (z * 4 + y) * 4, 4))
                else:
                    out.append((core * 64 + (z * 4 + y) * 4 + owner[X], 1))
        return out

    def halves(part, col, width):
        if len(part) == 1 and part[0][1] == 1:
            cut = (width // 2 + 127) // 128 * 128
            s = part[0][0]
            return [(s, 1, col, cut)], [(s, 1, col + cut, width - cut)]
        if len(part) == 1:
            s, n = part[0]
            return [(s, n // 2, col, width)], [(s + n // 2, n // 2, col, width)]
        m = len(part) // 2
        return [(s, n, col, width) for s, n in part[:m]], [(s, n, col, width) for s, n in part[m:]]

    def sem_h(p, phase, step, side):
        return r_h.at[((p * 3 + phase) * 2 + step) * 2 + side]

    def hidden_send(phase, step):
        for p, (order, col, width) in enumerate(PORTIONS):
            axis, free = order[phase], order[:phase]
            for side, d in enumerate((1, 3)):
                to = dev(shift(unit(axis, d)), core)
                if step == 0:
                    items = [(s, n, col, width) for s, n in runs(free, pos)]
                else:
                    items = halves(runs(free, shift(unit(axis, 4 - d))), col, width)[side]
                for s, n, c0, cw in items:
                    dst = hbuf.at[rows(s, n), pl.ds(c0, cw)]
                    src = hid_ref.at[:, pl.ds(c0, cw)] if phase == 0 and step == 0 else dst
                    send(src, dst, s_h.at[p], sem_h(p, phase, step, side), to)

    def hidden_wait(phase, step):
        for p, (order, col, width) in enumerate(PORTIONS):
            n = 4**phase
            for side in range(2):
                if step == 0:
                    ref = hbuf.at[pl.ds(0, n * 8), pl.ds(col, width)]
                elif phase == 0:
                    cut = (width // 2 + 127) // 128 * 128
                    ref = hbuf.at[pl.ds(0, 8), pl.ds(col, cut if side == 0 else width - cut)]
                else:
                    ref = hbuf.at[pl.ds(0, n * 4), pl.ds(col, width)]
                wait(ref, sem_h(p, phase, step, side))

    def columns(c, n):
        return pl.ds(pl.multiple_of(c * 1024, 1024), n * 1024)

    def first_hop(v):
        i = FIRST.index(v)
        to = shift(unit(ROUTES[v][0], v[ROUTES[v][0]]))
        send(w_ref.at[:, columns(chip(shift(v)) * 2, 2)], st_a.at[i], s_w.at[0], r_a.at[i], dev(to, core))

    def deliver(src_of, v, last):
        axis, d = last
        to = shift(unit(axis, d))
        origin = tuple((t - o) % 4 for t, o in zip(to, v))
        at = wbuf.at[pl.ds(pl.multiple_of((chip(origin) * 2 + core) * 32, 32), 32)]
        for c in (0, 1) if v[Z] == 1 or (v[Z] in (0, 2) and v[Y] == 1) else (1, 0):
            send(src_of(c), at, s_w.at[2], r_k.at[v[Z] * 4 + v[Y]], dev(to, c))

    def second_hop(v):
        i = FIRST.index(v)
        wait(st_a.at[i], r_a.at[i])
        axis = ROUTES[v][1]
        if len(ROUTES[v]) == 2:
            deliver(lambda c: st_a.at[i, :, pl.ds(c * 1024, 1024)], v, (axis, v[axis]))
        else:
            j = THREE_FLAT.index(v)
            send(st_a.at[i], st_b.at[j], s_w.at[1], r_b.at[j], dev(shift(unit(axis, v[axis])), core))

    def third_hop(v):
        j = THREE_FLAT.index(v)
        wait(st_b.at[j], r_b.at[j])
        axis = ROUTES[v][2]
        deliver(lambda c: st_b.at[j, :, pl.ds(c * 1024, 1024)], v, (axis, v[axis]))

    def single_hop(v):
        axis = ROUTES[v][0]
        deliver(lambda c: w_ref.at[:, columns(chip(shift(v)) * 2 + c, 1)], v, (axis, v[axis]))

    me = chip(pos) * 2 + core
    mine = wbuf.at[pl.ds(pl.multiple_of(me * 32, 32), 32)]
    slot = hbuf.at[rows(core * 64 + chip(pos))]
    pltpu.make_async_copy(hid_ref, slot, l_sem).start()
    pltpu.make_async_copy(w_ref.at[:, columns(me, 1)], mine, r_k.at[0]).start()

    for n, batch in enumerate(BATCHES):
        phase, step = divmod(n, 2)
        hidden_send(phase, step)
        for v in batch:
            if len(ROUTES[v]) == 1:
                single_hop(v)
            else:
                first_hop(v)
        if n == 0:
            wait(slot, l_sem)
        if n < 5:
            hidden_wait(phase, step)
    send(w_ref.at[:, columns(chip(pos) * 2 + 1 - core, 1)], mine, s_w.at[2], r_k.at[0], dev(pos, 1 - core))

    for v in THREE_FLAT:
        second_hop(v)
    for v in TWO_FLAT:
        second_hop(v)
    hidden_wait(2, 1)
    for p, (_, col, width) in enumerate(PORTIONS):
        half = hbuf.at[pl.ds(pl.multiple_of(core * 512, 512), 512), pl.ds(col, width)]
        send(half, half, s_x.at[p], r_x.at[p], dev(pos, 1 - core))
    for v in THREE_FLAT:
        third_hop(v)

    for p, (_, col, width) in enumerate(PORTIONS):
        wait(hbuf.at[pl.ds(0, 512), pl.ds(col, width)], r_x.at[p])

    def product(dz, dy, first):
        wait(wbuf.at[pl.ds(0, 256)], r_k.at[dz * 4 + dy])
        k0 = pl.multiple_of((((pos[Z] - dz) % 4) * 4 + (pos[Y] - dy) % 4) * 256, 256)
        for t in range(4):
            cols = pl.ds(t * 256, 256)
            part = jnp.dot(hbuf[:, pl.ds(k0, 256)], wbuf[pl.ds(k0, 256), cols], preferred_element_type=jnp.float32)
            if first:
                acc[:, cols] = part
            else:
                acc[:, cols] += part

    for n, line in enumerate(ORDER[: 16 - LATE]):
        product(*_mirror(line, core), n == 0)
    for dz, dy in [_mirror(line, core) for line in ORDER[16 - LATE :]]:
        wait(wbuf.at[pl.ds(0, 256)], r_k.at[dz * 4 + dy])

    wait(st_a, s_w.at[0])
    wait(st_b, s_w.at[1])
    wait(wbuf.at[pl.ds(0, 127 * 32)], s_w.at[2])
    for p, (_, col, width) in enumerate(PORTIONS):
        wait(hbuf.at[pl.ds(0, 63 * 8), pl.ds(col, width)], s_h.at[p])
        wait(hbuf.at[pl.ds(0, 512), pl.ds(col, width)], s_x.at[p])


def _mirror(line, core):
    return tuple(d if d in (0, 2) else d + core * (4 - 2 * d) for d in line)


def _finish(acc, hbuf, wbuf, out_ref, stage, sem):
    dp = lax.axis_index("dp")
    z, y = dp // 4, dp % 4
    core = lax.axis_index('tp') % 2
    lines = [_mirror(t, core) for t in ORDER[16 - LATE :]]
    starts = [pl.multiple_of((((z - dz) % 4) * 4 + (y - dy) % 4) * 256, 256) for dz, dy in lines]
    W = 256

    def step(t):
        cols = pl.ds(t * W, W)
        val = acc[:, cols]
        for k0 in starts:
            val += jnp.dot(hbuf[:, pl.ds(k0, 256)], wbuf[pl.ds(k0, 256), cols], preferred_element_type=jnp.float32)
        for i in range(64):
            pair = jnp.concatenate([val[i * 8 : i * 8 + 8], val[512 + i * 8 : 512 + i * 8 + 8]], axis=0)
            stage[i * 16 : i * 16 + 16, cols] = pair.astype(jnp.bfloat16)
        pltpu.make_async_copy(stage.at[:, cols], out_ref.at[:, cols], sem).start()

    for t in range(1024 // W):
        step(t)
    pltpu.make_async_copy(stage, out_ref, sem).wait()


def solution(mesh):
    def local_part(hid_blk, w_blk):
        dma = pltpu.SemaphoreType.DMA
        vm = pl.BlockSpec(memory_space=pltpu.VMEM)
        acc, hbuf, wbuf = pl.pallas_call(
            _kernel,
            out_shape=[pltpu.VMEM((1024, 1024), jnp.float32), pltpu.VMEM((1024, 4096), jnp.bfloat16), pltpu.VMEM((4096, 1024), jnp.bfloat16)],
            in_specs=[pl.BlockSpec(memory_space=pl.ANY)] * 2,
            out_specs=[vm] * 3,
            scratch_shapes=[
                pltpu.VMEM((len(FIRST), 32, 2048), jnp.bfloat16),
                pltpu.VMEM((len(THREE_FLAT), 32, 2048), jnp.bfloat16),
                dma((len(FIRST),)), dma((len(THREE_FLAT),)), dma((16,)), dma((3,)), dma((36,)), dma((3,)), dma((3,)), dma((3,)), dma,
            ],
            compiler_params=pltpu.CompilerParams(collective_id=0, has_side_effects=True, vmem_limit_bytes=38 * 2**20),
        )(hid_blk, w_blk)
        acc, hbuf, wbuf = (pltpu.with_memory_space_constraint(t, pltpu.VMEM) for t in (acc, hbuf, wbuf))
        return pl.pallas_call(
            _finish,
            out_shape=jax.ShapeDtypeStruct((1024, 1024), jnp.bfloat16),
            in_specs=[vm] * 3,
            out_specs=pl.BlockSpec(memory_space=pl.ANY),
            scratch_shapes=[pltpu.VMEM((1024, 1024), jnp.bfloat16), dma],
            compiler_params=pltpu.CompilerParams(vmem_limit_bytes=20 * 2**20),
        )(acc, hbuf, wbuf)

    return jax.shard_map(
        local_part,
        mesh=mesh,
        in_specs=(P(("dp", "tp"), None), P(("dp", "tp"), None)),
        out_specs=P(None, ("dp", "tp")),
        check_vma=False,
    )
```

```python
import functools

import jax
import jax.numpy as jnp
from jax import lax
from jax.experimental import pallas as pl
from jax.experimental.pallas import tpu as pltpu
from jax.sharding import PartitionSpec as P

MESH = pl.DeviceIdType.MESH
Z, Y, X = 0, 1, 2


def _turn(v):
    return (v[2], v[0], v[1])


def _neg(v):
    return tuple(-t % 4 for t in v)


def _last(v):
    z, y, x = v
    if sum(map(bool, v)) == 1:
        return next(a for a in range(3) if v[a])
    if x == 0:
        return Y if z == 2 or (y != 2 and z != y) else Z
    if z == 0 or y == 0:
        line, axis = (y, Y) if z == 0 else (z, Z)
        return axis if line != 2 and x in (2, line) else X
    if z == 2 and y == 2:
        return Y if x == 2 else X
    if z == 2:
        return Y if x in (2, y) else X
    if y == 2:
        return Z if x in (2, z) else X
    return Z if x == 2 else Y if x == z else X


def _route(v):
    last = _last(v)
    rest = [a for a in range(3) if v[a] and a != last]
    if len(rest) == 2:
        longer = [a for a in rest if v[a] == 2]
        if len(longer) == 1:
            first = longer[0]
        elif longer:
            first = X if X in rest else Z if v[X] == 1 else Y
        else:
            first = Z if last == Y else Y
        rest = [first] + [a for a in rest if a != first]
    return (*rest, last)


ALL = [(a, b, c) for a in range(4) for b in range(4) for c in range(4)][1:]
ROUTES = {v: _route(v) for v in ALL}
ONE = [v for v in ALL if len(ROUTES[v]) == 1]


def _lines(*lines):
    return [(*line, x) for line in lines for x in (1, 2, 3)]


G = dict(
    Q=_lines((2, 1), (2, 3), (1, 2), (3, 2)),
    T=_lines((2, 2)),
    P=_lines((1, 3), (3, 1)),
    R=_lines((1, 1), (3, 3)),
    A=_lines((0, 1), (0, 3)),
    B=_lines((0, 2)),
    C=_lines((2, 0)),
    D=_lines((1, 0), (3, 0)),
    E=[(a, b, 0) for a, b in ((2, 2), (2, 1), (2, 3), (1, 2), (3, 2), (1, 3), (3, 1), (1, 1), (3, 3))],
)
G["O"] = ONE
THREE_FLAT = G["T"] + G["Q"] + G["P"] + G["R"]
TWO_FLAT = G["A"] + G["D"] + G["B"] + G["C"] + G["E"]
GROUP = {v: n for n, g in enumerate('TQPRADBCE') for v in G[g]}
FIRST = THREE_FLAT + TWO_FLAT


ORDER = [(0, 0), (0, 1), (0, 3), (1, 0), (3, 0), (0, 2), (2, 0), (2, 2), (1, 2), (3, 2), (2, 1), (2, 3), (1, 3), (3, 1), (1, 1), (3, 3)]
LATE = 1
SCHEDULE = (
    "H0", "1Q", "SS", "W0",
    "H1", "1O", "1T", "W1",
    "H2", "1P", "1R", "W2",
    "H3", "1A", "1B", "1C", "1D", "W3",
    "H4", "1E", "2T", "2Q", "W4",
    "H5", "CC", "2P", "2R", "2A", "2D", "2B", "2C",
    "2E", "3T", "3Q", "W5",
    "XX", "3P", "3R",
)
PORTIONS = (((X, Y, Z), 0, 1280), ((Y, Z, X), 1280, 1408), ((Z, X, Y), 2688, 1408))


def _kernel(hid_ref, w_ref, acc, hbuf, wbuf, st_a, st_b, r_a, r_b, r_k, s_w, r_h, s_h, r_x, s_x, l_sem):
    dp, tp = lax.axis_index("dp"), lax.axis_index("tp")
    pos, core = (dp // 4, dp % 4, tp // 2), tp % 2

    def shift(v):
        return tuple((p + d) % 4 if d else p for p, d in zip(pos, v))

    def dev(p, c):
        return (p[Z] * 4 + p[Y], p[X] * 2 + c)

    def chip(p):
        return (p[Z] * 4 + p[Y]) * 4 + p[X]

    def unit(axis, d):
        return tuple(d if a == axis else 0 for a in range(3))

    def send(src, dst, ssem, rsem, to):
        pltpu.make_async_remote_copy(
            src_ref=src, dst_ref=dst, send_sem=ssem, recv_sem=rsem, device_id=to, device_id_type=MESH
        ).start()

    def wait(ref, sem):
        pltpu.make_async_copy(ref, ref, sem).wait()

    barrier = pltpu.get_barrier_semaphore()
    peers = [dev(pos, 1 - core)]
    for axis in (X, Y, Z):
        for d in (1, 3, 2):
            for c in (core, 1 - core):
                peers.append(dev(shift(unit(axis, d)), c))
    for peer in peers:
        pl.semaphore_signal(barrier, inc=1, device_id=peer, device_id_type=MESH)
    pl.semaphore_wait(barrier, len(peers))

    def rows(slot, n=1):
        return pl.ds(pl.multiple_of(slot * 8, 8), n * 8)

    def runs(free, owner):
        out = []
        for z in range(4) if Z in free else (owner[Z],):
            for y in range(4) if Y in free and not (Y in free and X in free) else (owner[Y],):
                if X in free and Y in free:
                    out.append((core * 64 + z * 16, 16))
                elif X in free:
                    out.append((core * 64 + (z * 4 + y) * 4, 4))
                else:
                    out.append((core * 64 + (z * 4 + y) * 4 + owner[X], 1))
        return out

    def halves(part, col, width):
        if len(part) == 1 and part[0][1] == 1:
            cut = (width // 2 + 127) // 128 * 128
            s = part[0][0]
            return [(s, 1, col, cut)], [(s, 1, col + cut, width - cut)]
        if len(part) == 1:
            s, n = part[0]
            return [(s, n // 2, col, width)], [(s + n // 2, n // 2, col, width)]
        m = len(part) // 2
        return [(s, n, col, width) for s, n in part[:m]], [(s, n, col, width) for s, n in part[m:]]

    def hidden_send(phase, step):
        for p, (order, col, width) in enumerate(PORTIONS):
            axis, free = order[phase], order[:phase]
            for side, d in enumerate((1, 3)):
                to = dev(shift(unit(axis, d)), core)
                if step == 0:
                    items = [(s, n, col, width) for s, n in runs(free, pos)]
                else:
                    items = halves(runs(free, shift(unit(axis, 4 - d))), col, width)[side]
                for s, n, c0, cw in items:
                    dst = hbuf.at[rows(s, n), pl.ds(c0, cw)]
                    src = hid_ref.at[:, pl.ds(c0, cw)] if phase == 0 and step == 0 else dst
                    send(src, dst, s_h, r_h.at[phase * 2 + step], to)

    def hidden_wait(phase, step):
        n = 4**phase * (2, 1)[step]
        wait(hbuf.at[pl.ds(0, n * 8)], r_h.at[phase * 2 + step])

    def columns(c, n):
        return pl.ds(pl.multiple_of(c * 1024, 1024), n * 1024)

    def first_hop(v):
        i = FIRST.index(v)
        to = shift(unit(ROUTES[v][0], v[ROUTES[v][0]]))
        send(w_ref.at[:, columns(chip(shift(v)) * 2, 2)], st_a.at[i], s_w.at[0], r_a.at[GROUP[v]], dev(to, core))

    def deliver(src_of, v, last):
        axis, d = last
        to = shift(unit(axis, d))
        origin = tuple((t - o) % 4 for t, o in zip(to, v))
        at = wbuf.at[pl.ds(pl.multiple_of((chip(origin) * 2 + core) * 32, 32), 32)]
        for c in (0, 1) if v[Z] == 1 or (v[Z] in (0, 2) and v[Y] == 1) else (1, 0):
            send(src_of(c), at, s_w.at[2], r_k.at[v[Z] * 4 + v[Y]], dev(to, c))

    def second_hop(v):
        i = FIRST.index(v)
        axis = ROUTES[v][1]
        if len(ROUTES[v]) == 2:
            deliver(lambda c: st_a.at[i, :, pl.ds(c * 1024, 1024)], v, (axis, v[axis]))
        else:
            j = THREE_FLAT.index(v)
            send(st_a.at[i], st_b.at[j], s_w.at[1], r_b.at[GROUP[v]], dev(shift(unit(axis, v[axis])), core))

    def third_hop(v):
        j = THREE_FLAT.index(v)
        axis = ROUTES[v][2]
        deliver(lambda c: st_b.at[j, :, pl.ds(c * 1024, 1024)], v, (axis, v[axis]))

    def single_hop(v):
        axis = ROUTES[v][0]
        deliver(lambda c: w_ref.at[:, columns(chip(shift(v)) * 2 + c, 1)], v, (axis, v[axis]))

    me = chip(pos) * 2 + core
    mine = wbuf.at[pl.ds(pl.multiple_of(me * 32, 32), 32)]
    slot = hbuf.at[rows(core * 64 + chip(pos))]
    pltpu.make_async_copy(hid_ref, slot, l_sem).start()
    pltpu.make_async_copy(w_ref.at[:, columns(me, 1)], mine, r_k.at[0]).start()

    for kind, which in SCHEDULE:
        if kind == "H":
            hidden_send(*divmod(int(which), 2))
        elif kind == "W":
            hidden_wait(*divmod(int(which), 2))
        elif kind == "S":
            wait(slot, l_sem)
        elif kind == "1":
            for v in G[which]:
                if len(ROUTES[v]) == 1:
                    single_hop(v)
                else:
                    first_hop(v)
        elif kind == "2":
            wait(st_a.at[pl.ds(FIRST.index(G[which][0]), len(G[which]))], r_a.at[GROUP[G[which][0]]])
            for v in G[which]:
                second_hop(v)
        elif kind == "3":
            wait(st_b.at[pl.ds(FIRST.index(G[which][0]), len(G[which]))], r_b.at[GROUP[G[which][0]]])
            for v in G[which]:
                third_hop(v)
        elif kind == "C":
            send(w_ref.at[:, columns(chip(pos) * 2 + 1 - core, 1)], mine, s_w.at[2], r_k.at[0], dev(pos, 1 - core))
        else:
            half = hbuf.at[pl.ds(pl.multiple_of(core * 512, 512), 512)]
            send(half, half, s_x, r_x, dev(pos, 1 - core))

    wait(hbuf.at[pl.ds(0, 512)], r_x)

    def product(dz, dy, first):
        wait(wbuf.at[pl.ds(0, 256)], r_k.at[dz * 4 + dy])
        k0 = pl.multiple_of((((pos[Z] - dz) % 4) * 4 + (pos[Y] - dy) % 4) * 256, 256)
        for t in range(4):
            cols = pl.ds(t * 256, 256)
            part = jnp.dot(hbuf[:, pl.ds(k0, 256)], wbuf[pl.ds(k0, 256), cols], preferred_element_type=jnp.float32)
            if first:
                acc[:, cols] = part
            else:
                acc[:, cols] += part

    for n, line in enumerate(ORDER[: 16 - LATE]):
        product(*_mirror(line, core), n == 0)
    for dz, dy in [_mirror(line, core) for line in ORDER[16 - LATE :]]:
        wait(wbuf.at[pl.ds(0, 256)], r_k.at[dz * 4 + dy])

    wait(st_a, s_w.at[0])
    wait(st_b, s_w.at[1])
    wait(wbuf.at[pl.ds(0, 127 * 32)], s_w.at[2])
    wait(hbuf.at[pl.ds(0, 63 * 8)], s_h)
    wait(hbuf.at[pl.ds(0, 512)], s_x)


def _mirror(line, core):
    return tuple(d if d in (0, 2) else d + core * (4 - 2 * d) for d in line)


def _finish(acc, hbuf, wbuf, out_ref, stage, sem):
    dp = lax.axis_index("dp")
    z, y = dp // 4, dp % 4
    core = lax.axis_index('tp') % 2
    lines = [_mirror(t, core) for t in ORDER[16 - LATE :]]
    starts = [pl.multiple_of((((z - dz) % 4) * 4 + (y - dy) % 4) * 256, 256) for dz, dy in lines]
    W = 256

    def step(t):
        cols = pl.ds(t * W, W)
        val = acc[:, cols]
        for k0 in starts:
            val += jnp.dot(hbuf[:, pl.ds(k0, 256)], wbuf[pl.ds(k0, 256), cols], preferred_element_type=jnp.float32)
        for i in range(64):
            pair = jnp.concatenate([val[i * 8 : i * 8 + 8], val[512 + i * 8 : 512 + i * 8 + 8]], axis=0)
            stage[i * 16 : i * 16 + 16, cols] = pair.astype(jnp.bfloat16)
        pltpu.make_async_copy(stage.at[:, cols], out_ref.at[:, cols], sem).start()

    for t in range(1024 // W):
        step(t)
    pltpu.make_async_copy(stage, out_ref, sem).wait()


def solution(mesh):
    def local_part(hid_blk, w_blk):
        dma = pltpu.SemaphoreType.DMA
        vm = pl.BlockSpec(memory_space=pltpu.VMEM)
        acc, hbuf, wbuf = pl.pallas_call(
            _kernel,
            out_shape=[pltpu.VMEM((1024, 1024), jnp.float32), pltpu.VMEM((1024, 4096), jnp.bfloat16), pltpu.VMEM((4096, 1024), jnp.bfloat16)],
            in_specs=[pl.BlockSpec(memory_space=pl.ANY)] * 2,
            out_specs=[vm] * 3,
            scratch_shapes=[
                pltpu.VMEM((len(FIRST), 32, 2048), jnp.bfloat16),
                pltpu.VMEM((len(THREE_FLAT), 32, 2048), jnp.bfloat16),
                dma((9,)), dma((4,)), dma((16,)), dma((3,)), dma((6,)), dma, dma, dma, dma,
            ],
            compiler_params=pltpu.CompilerParams(collective_id=0, has_side_effects=True, vmem_limit_bytes=38 * 2**20),
        )(hid_blk, w_blk)
        acc, hbuf, wbuf = (pltpu.with_memory_space_constraint(t, pltpu.VMEM) for t in (acc, hbuf, wbuf))
        return pl.pallas_call(
            _finish,
            out_shape=jax.ShapeDtypeStruct((1024, 1024), jnp.bfloat16),
            in_specs=[vm] * 3,
            out_specs=pl.BlockSpec(memory_space=pl.ANY),
            scratch_shapes=[pltpu.VMEM((1024, 1024), jnp.bfloat16), dma],
            compiler_params=pltpu.CompilerParams(vmem_limit_bytes=20 * 2**20),
        )(acc, hbuf, wbuf)

    return jax.shard_map(
        local_part,
        mesh=mesh,
        in_specs=(P(("dp", "tp"), None), P(("dp", "tp"), None)),
        out_specs=P(None, ("dp", "tp")),
        check_vma=False,
    )
```

```python
import functools

import jax
import jax.numpy as jnp
from jax import lax
from jax.experimental import pallas as pl
from jax.experimental.pallas import tpu as pltpu
from jax.sharding import PartitionSpec as P

MESH = pl.DeviceIdType.MESH
Z, Y, X = 0, 1, 2


def _turn(v):
    return (v[2], v[0], v[1])


def _neg(v):
    return tuple(-t % 4 for t in v)


def _last(v):
    z, y, x = v
    if sum(map(bool, v)) == 1:
        return next(a for a in range(3) if v[a])
    if x == 0:
        return Y if z == 2 or (y != 2 and z != y) else Z
    if z == 0 or y == 0:
        line, axis = (y, Y) if z == 0 else (z, Z)
        return axis if line != 2 and x in (2, line) else X
    if z == 2 and y == 2:
        return Y if x == 2 else X
    if z == 2:
        return Y if x in (2, y) else X
    if y == 2:
        return Z if x in (2, z) else X
    return Z if x == 2 else Y if x == z else X


def _route(v):
    last = _last(v)
    rest = [a for a in range(3) if v[a] and a != last]
    if len(rest) == 2:
        longer = [a for a in rest if v[a] == 2]
        if len(longer) == 1:
            first = longer[0]
        elif longer:
            first = X if X in rest else Z if v[X] == 1 else Y
        else:
            first = Z if last == Y else Y
        rest = [first] + [a for a in rest if a != first]
    return (*rest, last)


ALL = [(a, b, c) for a in range(4) for b in range(4) for c in range(4)][1:]
ROUTES = {v: _route(v) for v in ALL}
ONE = [v for v in ALL if len(ROUTES[v]) == 1]


def _lines(*lines):
    return [(*line, x) for line in lines for x in (1, 2, 3)]


G = dict(
    Q=_lines((2, 1), (2, 3), (1, 2), (3, 2)),
    T=_lines((2, 2)),
    P=_lines((1, 3), (3, 1)),
    R=_lines((1, 1), (3, 3)),
    A=_lines((0, 1), (0, 3)),
    B=_lines((0, 2)),
    C=_lines((2, 0)),
    D=_lines((1, 0), (3, 0)),
    E=[(a, b, 0) for a, b in ((2, 2), (2, 1), (2, 3), (1, 2), (3, 2), (1, 3), (3, 1), (1, 1), (3, 3))],
)
G["O"] = ONE
THREE_FLAT = G["T"] + G["Q"] + G["P"] + G["R"]
TWO_FLAT = G["A"] + G["D"] + G["B"] + G["C"] + G["E"]
GROUP = {v: n for n, g in enumerate('TQPRADBCE') for v in G[g]}
FIRST = THREE_FLAT + TWO_FLAT


ORDER = [(0, 0), (0, 1), (0, 3), (1, 0), (3, 0), (0, 2), (2, 0), (2, 2), (1, 2), (3, 2), (2, 1), (2, 3), (1, 3), (3, 1), (1, 1), (3, 3)]
LATE = 1
SCHEDULE = (
    "H0", "1Q", "SS", "W0",
    "H1", "1O", "1T", "W1",
    "H2", "1P", "1R", "W2",
    "H3", "1A", "1B", "1C", "1D", "W3",
    "H4", "1E", "2T", "2Q", "W4",
    "H5", "CC", "2P", "2R", "2A", "2D", "2B", "2C",
    "2E", "3T", "3Q", "W5",
    "XX", "3P", "3R",
)
PORTIONS = (((X, Y, Z), 0, 1408), ((Y, Z, X), 1408, 1408), ((Z, X, Y), 2816, 1280))


def _kernel(hid_ref, w_ref, acc, hbuf, wbuf, st_a, st_b, r_a, r_b, r_k, s_w, r_h, s_h, r_x, s_x, l_sem):
    dp, tp = lax.axis_index("dp"), lax.axis_index("tp")
    pos, core = (dp // 4, dp % 4, tp // 2), tp % 2

    def shift(v):
        return tuple((p + d) % 4 if d else p for p, d in zip(pos, v))

    def dev(p, c):
        return (p[Z] * 4 + p[Y], p[X] * 2 + c)

    def chip(p):
        return (p[Z] * 4 + p[Y]) * 4 + p[X]

    def unit(axis, d):
        return tuple(d if a == axis else 0 for a in range(3))

    def send(src, dst, ssem, rsem, to):
        pltpu.make_async_remote_copy(
            src_ref=src, dst_ref=dst, send_sem=ssem, recv_sem=rsem, device_id=to, device_id_type=MESH
        ).start()

    def wait(ref, sem):
        pltpu.make_async_copy(ref, ref, sem).wait()

    barrier = pltpu.get_barrier_semaphore()
    peers = [dev(pos, 1 - core)]
    for axis in (X, Y, Z):
        for d in (1, 3, 2):
            for c in (core, 1 - core):
                peers.append(dev(shift(unit(axis, d)), c))
    for peer in peers:
        pl.semaphore_signal(barrier, inc=1, device_id=peer, device_id_type=MESH)
    pl.semaphore_wait(barrier, len(peers))

    def rows(slot, n=1):
        return pl.ds(pl.multiple_of(slot * 8, 8), n * 8)

    def runs(free, owner):
        out = []
        for z in range(4) if Z in free else (owner[Z],):
            for y in range(4) if Y in free and not (Y in free and X in free) else (owner[Y],):
                if X in free and Y in free:
                    out.append((core * 64 + z * 16, 16))
                elif X in free:
                    out.append((core * 64 + (z * 4 + y) * 4, 4))
                else:
                    out.append((core * 64 + (z * 4 + y) * 4 + owner[X], 1))
        return out

    def halves(part, col, width):
        if len(part) == 1 and part[0][1] == 1:
            cut = (width // 2 + 127) // 128 * 128
            s = part[0][0]
            return [(s, 1, col, cut)], [(s, 1, col + cut, width - cut)]
        if len(part) == 1:
            s, n = part[0]
            return [(s, n // 2, col, width)], [(s + n // 2, n // 2, col, width)]
        m = len(part) // 2
        return [(s, n, col, width) for s, n in part[:m]], [(s, n, col, width) for s, n in part[m:]]

    def hidden_send(phase, step):
        for p, (order, col, width) in enumerate(PORTIONS):
            axis, free = order[phase], order[:phase]
            for side, d in enumerate((1, 3)):
                to = dev(shift(unit(axis, d)), core)
                if step == 0:
                    items = [(s, n, col, width) for s, n in runs(free, pos)]
                else:
                    items = halves(runs(free, shift(unit(axis, 4 - d))), col, width)[side]
                for s, n, c0, cw in items:
                    dst = hbuf.at[rows(s, n), pl.ds(c0, cw)]
                    src = hid_ref.at[:, pl.ds(c0, cw)] if phase == 0 and step == 0 else dst
                    send(src, dst, s_h, r_h.at[phase * 2 + step], to)

    def hidden_wait(phase, step):
        n = 4**phase * (2, 1)[step]
        wait(hbuf.at[pl.ds(0, n * 8)], r_h.at[phase * 2 + step])

    def columns(c, n):
        return pl.ds(pl.multiple_of(c * 1024, 1024), n * 1024)

    def first_hop(v):
        i = FIRST.index(v)
        to = shift(unit(ROUTES[v][0], v[ROUTES[v][0]]))
        send(w_ref.at[:, columns(chip(shift(v)) * 2, 2)], st_a.at[i], s_w.at[0], r_a.at[GROUP[v]], dev(to, core))

    def deliver(src_of, v, last):
        axis, d = last
        to = shift(unit(axis, d))
        origin = tuple((t - o) % 4 for t, o in zip(to, v))
        at = wbuf.at[pl.ds(pl.multiple_of((chip(origin) * 2 + core) * 32, 32), 32)]
        for c in (0, 1) if v[Z] == 1 or (v[Z] in (0, 2) and v[Y] == 1) else (1, 0):
            send(src_of(c), at, s_w.at[2], r_k.at[v[Z] * 4 + v[Y]], dev(to, c))

    def second_hop(v):
        i = FIRST.index(v)
        axis = ROUTES[v][1]
        if len(ROUTES[v]) == 2:
            deliver(lambda c: st_a.at[i, :, pl.ds(c * 1024, 1024)], v, (axis, v[axis]))
        else:
            j = THREE_FLAT.index(v)
            send(st_a.at[i], st_b.at[j], s_w.at[1], r_b.at[GROUP[v]], dev(shift(unit(axis, v[axis])), core))

    def third_hop(v):
        j = THREE_FLAT.index(v)
        axis = ROUTES[v][2]
        deliver(lambda c: st_b.at[j, :, pl.ds(c * 1024, 1024)], v, (axis, v[axis]))

    def single_hop(v):
        axis = ROUTES[v][0]
        deliver(lambda c: w_ref.at[:, columns(chip(shift(v)) * 2 + c, 1)], v, (axis, v[axis]))

    me = chip(pos) * 2 + core
    mine = wbuf.at[pl.ds(pl.multiple_of(me * 32, 32), 32)]
    slot = hbuf.at[rows(core * 64 + chip(pos))]
    pltpu.make_async_copy(hid_ref, slot, l_sem).start()
    pltpu.make_async_copy(w_ref.at[:, columns(me, 1)], mine, r_k.at[0]).start()

    for kind, which in SCHEDULE:
        if kind == "H":
            hidden_send(*divmod(int(which), 2))
        elif kind == "W":
            hidden_wait(*divmod(int(which), 2))
        elif kind == "S":
            wait(slot, l_sem)
        elif kind == "1":
            for v in G[which]:
                if len(ROUTES[v]) == 1:
                    single_hop(v)
                else:
                    first_hop(v)
        elif kind == "2":
            wait(st_a.at[pl.ds(FIRST.index(G[which][0]), len(G[which]))], r_a.at[GROUP[G[which][0]]])
            for v in G[which]:
                second_hop(v)
        elif kind == "3":
            wait(st_b.at[pl.ds(FIRST.index(G[which][0]), len(G[which]))], r_b.at[GROUP[G[which][0]]])
            for v in G[which]:
                third_hop(v)
        elif kind == "C":
            send(w_ref.at[:, columns(chip(pos) * 2 + 1 - core, 1)], mine, s_w.at[2], r_k.at[0], dev(pos, 1 - core))
        else:
            half = hbuf.at[pl.ds(pl.multiple_of(core * 512, 512), 512)]
            send(half, half, s_x, r_x, dev(pos, 1 - core))

    wait(hbuf.at[pl.ds(0, 512)], r_x)

    def product(dz, dy, first):
        wait(wbuf.at[pl.ds(0, 256)], r_k.at[dz * 4 + dy])
        k0 = pl.multiple_of((((pos[Z] - dz) % 4) * 4 + (pos[Y] - dy) % 4) * 256, 256)
        for t in range(4):
            cols = pl.ds(t * 256, 256)
            part = jnp.dot(hbuf[:, pl.ds(k0, 256)], wbuf[pl.ds(k0, 256), cols], preferred_element_type=jnp.float32)
            if first:
                acc[:, cols] = part
            else:
                acc[:, cols] += part

    for n, line in enumerate(ORDER[: 16 - LATE]):
        product(*_mirror(line, core), n == 0)
    for dz, dy in [_mirror(line, core) for line in ORDER[16 - LATE :]]:
        wait(wbuf.at[pl.ds(0, 256)], r_k.at[dz * 4 + dy])

    wait(st_a, s_w.at[0])
    wait(st_b, s_w.at[1])
    wait(wbuf.at[pl.ds(0, 127 * 32)], s_w.at[2])
    wait(hbuf.at[pl.ds(0, 63 * 8)], s_h)
    wait(hbuf.at[pl.ds(0, 512)], s_x)


def _mirror(line, core):
    return tuple(d if d in (0, 2) else d + core * (4 - 2 * d) for d in line)


def _finish(acc, hbuf, wbuf, out_ref, stage, sem):
    dp = lax.axis_index("dp")
    z, y = dp // 4, dp % 4
    core = lax.axis_index('tp') % 2
    lines = [_mirror(t, core) for t in ORDER[16 - LATE :]]
    starts = [pl.multiple_of((((z - dz) % 4) * 4 + (y - dy) % 4) * 256, 256) for dz, dy in lines]
    W = 512

    def step(t):
        cols = pl.ds(t * W, W)
        val = acc[:, cols]
        for k0 in starts:
            val += jnp.dot(hbuf[:, pl.ds(k0, 256)], wbuf[pl.ds(k0, 256), cols], preferred_element_type=jnp.float32)
        for i in range(64):
            pair = jnp.concatenate([val[i * 8 : i * 8 + 8], val[512 + i * 8 : 512 + i * 8 + 8]], axis=0)
            stage[i * 16 : i * 16 + 16, cols] = pair.astype(jnp.bfloat16)
        pltpu.make_async_copy(stage.at[:, cols], out_ref.at[:, cols], sem).start()

    for t in range(1024 // W):
        step(t)
    pltpu.make_async_copy(stage, out_ref, sem).wait()


def solution(mesh):
    def local_part(hid_blk, w_blk):
        dma = pltpu.SemaphoreType.DMA
        vm = pl.BlockSpec(memory_space=pltpu.VMEM)
        acc, hbuf, wbuf = pl.pallas_call(
            _kernel,
            out_shape=[pltpu.VMEM((1024, 1024), jnp.float32), pltpu.VMEM((1024, 4096), jnp.bfloat16), pltpu.VMEM((4096, 1024), jnp.bfloat16)],
            in_specs=[pl.BlockSpec(memory_space=pl.ANY)] * 2,
            out_specs=[vm] * 3,
            scratch_shapes=[
                pltpu.VMEM((len(FIRST), 32, 2048), jnp.bfloat16),
                pltpu.VMEM((len(THREE_FLAT), 32, 2048), jnp.bfloat16),
                dma((9,)), dma((4,)), dma((16,)), dma((3,)), dma((6,)), dma, dma, dma, dma,
            ],
            compiler_params=pltpu.CompilerParams(collective_id=0, has_side_effects=True, vmem_limit_bytes=38 * 2**20),
        )(hid_blk, w_blk)
        acc, hbuf, wbuf = (pltpu.with_memory_space_constraint(t, pltpu.VMEM) for t in (acc, hbuf, wbuf))
        return pl.pallas_call(
            _finish,
            out_shape=jax.ShapeDtypeStruct((1024, 1024), jnp.bfloat16),
            in_specs=[vm] * 3,
            out_specs=pl.BlockSpec(memory_space=pl.ANY),
            scratch_shapes=[pltpu.VMEM((1024, 1024), jnp.bfloat16), dma],
            compiler_params=pltpu.CompilerParams(vmem_limit_bytes=20 * 2**20),
        )(acc, hbuf, wbuf)

    return jax.shard_map(
        local_part,
        mesh=mesh,
        in_specs=(P(("dp", "tp"), None), P(("dp", "tp"), None)),
        out_specs=P(None, ("dp", "tp")),
        check_vma=False,
    )
```

```python
import functools

import jax
import jax.numpy as jnp
from jax import lax
from jax.experimental import pallas as pl
from jax.experimental.pallas import tpu as pltpu
from jax.sharding import PartitionSpec as P

MESH = pl.DeviceIdType.MESH
Z, Y, X = 0, 1, 2


def _turn(v):
    return (v[2], v[0], v[1])


def _neg(v):
    return tuple(-t % 4 for t in v)


def _last(v):
    z, y, x = v
    if sum(map(bool, v)) == 1:
        return next(a for a in range(3) if v[a])
    if x == 0:
        return Y if z == 2 or (y != 2 and z != y) else Z
    if z == 0 or y == 0:
        line, axis = (y, Y) if z == 0 else (z, Z)
        return axis if line != 2 and x in (2, line) else X
    if z == 2 and y == 2:
        return Y if x == 2 else X
    if z == 2:
        return Y if x in (2, y) else X
    if y == 2:
        return Z if x in (2, z) else X
    return Z if x == 2 else Y if x == z else X


def _route(v):
    last = _last(v)
    rest = [a for a in range(3) if v[a] and a != last]
    if len(rest) == 2:
        longer = [a for a in rest if v[a] == 2]
        if len(longer) == 1:
            first = longer[0]
        elif longer:
            first = X if X in rest else Z if v[X] == 1 else Y
        else:
            first = Z if last == Y else Y
        rest = [first] + [a for a in rest if a != first]
    return (*rest, last)


ALL = [(a, b, c) for a in range(4) for b in range(4) for c in range(4)][1:]
ROUTES = {v: _route(v) for v in ALL}
ONE = [v for v in ALL if len(ROUTES[v]) == 1]


def _lines(*lines):
    return [(*line, x) for line in lines for x in (1, 2, 3)]


G = dict(
    Q=_lines((2, 1), (2, 3), (1, 2), (3, 2)),
    T=_lines((2, 2)),
    P=_lines((1, 3), (3, 1)),
    R=_lines((1, 1), (3, 3)),
    A=_lines((0, 1), (0, 3)),
    B=_lines((0, 2)),
    C=_lines((2, 0)),
    D=_lines((1, 0), (3, 0)),
    E=[(a, b, 0) for a, b in ((2, 2), (2, 1), (2, 3), (1, 2), (3, 2), (1, 3), (3, 1), (1, 1), (3, 3))],
)
G["O"] = ONE
THREE_FLAT = G["T"] + G["Q"] + G["P"] + G["R"]
TWO_FLAT = G["A"] + G["D"] + G["B"] + G["C"] + G["E"]
G["V"] = G["P"] + G["R"]
G["F"] = G["A"] + G["D"] + G["B"] + G["C"]
GROUP = {v: n for n, g in enumerate("TQVFE") for v in G[g]}
GROUP_B = {v: n for n, g in enumerate("TQPR") for v in G[g]}
FIRST = THREE_FLAT + TWO_FLAT


ORDER = [(0, 0), (0, 1), (0, 3), (1, 0), (3, 0), (0, 2), (2, 0), (2, 2), (1, 2), (3, 2), (2, 1), (2, 3), (1, 3), (3, 1), (1, 1), (3, 3)]
LATE = 1
SCHEDULE = (
    "H0", "1Q", "SS", "W0",
    "H1", "1O", "1T", "W1",
    "H2", "1P", "1R", "W2",
    "H3", "1A", "1B", "1C", "1D", "W3",
    "H4", "1E", "2T", "2Q", "W4",
    "H5", "CC", "2V", "2F", "2E", "3T", "3Q", "W5",
    "XX", "3P", "3R",
)
PORTIONS = (((X, Y, Z), 0, 1408), ((Y, Z, X), 1408, 1408), ((Z, X, Y), 2816, 1280))


def _kernel(hid_ref, w_ref, acc, hbuf, wbuf, st_a, st_b, r_a, r_b, r_k, s_w, r_h, s_h, r_x, l_sem):
    dp, tp = lax.axis_index("dp"), lax.axis_index("tp")
    pos, core = (dp // 4, dp % 4, tp // 2), tp % 2

    def shift(v):
        return tuple((p + d) % 4 if d else p for p, d in zip(pos, v))

    def dev(p, c):
        return (p[Z] * 4 + p[Y], p[X] * 2 + c)

    def chip(p):
        return (p[Z] * 4 + p[Y]) * 4 + p[X]

    def unit(axis, d):
        return tuple(d if a == axis else 0 for a in range(3))

    def send(src, dst, ssem, rsem, to):
        pltpu.make_async_remote_copy(
            src_ref=src, dst_ref=dst, send_sem=ssem, recv_sem=rsem, device_id=to, device_id_type=MESH
        ).start()

    def wait(ref, sem):
        pltpu.make_async_copy(ref, ref, sem).wait()

    barrier = pltpu.get_barrier_semaphore()
    peers = [dev(pos, 1 - core)]
    for axis in (X, Y, Z):
        for d in (1, 3, 2):
            for c in (core, 1 - core):
                peers.append(dev(shift(unit(axis, d)), c))
    for peer in peers:
        pl.semaphore_signal(barrier, inc=1, device_id=peer, device_id_type=MESH)
    pl.semaphore_wait(barrier, len(peers))

    def rows(slot, n=1):
        return pl.ds(pl.multiple_of(slot * 8, 8), n * 8)

    def runs(free, owner):
        out = []
        for z in range(4) if Z in free else (owner[Z],):
            for y in range(4) if Y in free and not (Y in free and X in free) else (owner[Y],):
                if X in free and Y in free:
                    out.append((core * 64 + z * 16, 16))
                elif X in free:
                    out.append((core * 64 + (z * 4 + y) * 4, 4))
                else:
                    out.append((core * 64 + (z * 4 + y) * 4 + owner[X], 1))
        return out

    def halves(part, col, width):
        if len(part) == 1 and part[0][1] == 1:
            cut = (width // 2 + 127) // 128 * 128
            s = part[0][0]
            return [(s, 1, col, cut)], [(s, 1, col + cut, width - cut)]
        if len(part) == 1:
            s, n = part[0]
            return [(s, n // 2, col, width)], [(s + n // 2, n // 2, col, width)]
        m = len(part) // 2
        return [(s, n, col, width) for s, n in part[:m]], [(s, n, col, width) for s, n in part[m:]]

    def hidden_send(phase, step):
        for p, (order, col, width) in enumerate(PORTIONS):
            axis, free = order[phase], order[:phase]
            for side, d in enumerate((1, 3)):
                to = dev(shift(unit(axis, d)), core)
                if step == 0:
                    items = [(s, n, col, width) for s, n in runs(free, pos)]
                else:
                    items = halves(runs(free, shift(unit(axis, 4 - d))), col, width)[side]
                for s, n, c0, cw in items:
                    dst = hbuf.at[rows(s, n), pl.ds(c0, cw)]
                    src = hid_ref.at[:, pl.ds(c0, cw)] if phase == 0 and step == 0 else dst
                    send(src, dst, s_h, r_h.at[phase * 2 + step], to)

    def hidden_wait(phase, step):
        n = 4**phase * (2, 1)[step]
        wait(hbuf.at[pl.ds(0, n * 8)], r_h.at[phase * 2 + step])

    def columns(c, n):
        return pl.ds(pl.multiple_of(c * 1024, 1024), n * 1024)

    def first_hop(v):
        i = FIRST.index(v)
        to = shift(unit(ROUTES[v][0], v[ROUTES[v][0]]))
        send(w_ref.at[:, columns(chip(shift(v)) * 2, 2)], st_a.at[i], s_w.at[0], r_a.at[GROUP[v]], dev(to, core))

    def deliver(src_of, v, last):
        axis, d = last
        to = shift(unit(axis, d))
        origin = tuple((t - o) % 4 for t, o in zip(to, v))
        at = wbuf.at[pl.ds(pl.multiple_of((chip(origin) * 2 + core) * 32, 32), 32)]
        for c in (0, 1) if v[Z] == 1 or (v[Z] in (0, 2) and v[Y] == 1) else (1, 0):
            send(src_of(c), at, s_w.at[2], r_k.at[v[Z] * 4 + v[Y]], dev(to, c))

    def second_hop(v):
        i = FIRST.index(v)
        axis = ROUTES[v][1]
        if len(ROUTES[v]) == 2:
            deliver(lambda c: st_a.at[i, :, pl.ds(c * 1024, 1024)], v, (axis, v[axis]))
        else:
            j = THREE_FLAT.index(v)
            send(st_a.at[i], st_b.at[j], s_w.at[1], r_b.at[GROUP_B[v]], dev(shift(unit(axis, v[axis])), core))

    def third_hop(v):
        j = THREE_FLAT.index(v)
        axis = ROUTES[v][2]
        deliver(lambda c: st_b.at[j, :, pl.ds(c * 1024, 1024)], v, (axis, v[axis]))

    def single_hop(v):
        axis = ROUTES[v][0]
        deliver(lambda c: w_ref.at[:, columns(chip(shift(v)) * 2 + c, 1)], v, (axis, v[axis]))

    me = chip(pos) * 2 + core
    mine = wbuf.at[pl.ds(pl.multiple_of(me * 32, 32), 32)]
    slot = hbuf.at[rows(core * 64 + chip(pos))]
    pltpu.make_async_copy(hid_ref, slot, l_sem).start()
    pltpu.make_async_copy(w_ref.at[:, columns(me, 1)], mine, r_k.at[0]).start()

    for kind, which in SCHEDULE:
        if kind == "H":
            hidden_send(*divmod(int(which), 2))
        elif kind == "W":
            hidden_wait(*divmod(int(which), 2))
        elif kind == "S":
            wait(slot, l_sem)
        elif kind == "1":
            for v in G[which]:
                if len(ROUTES[v]) == 1:
                    single_hop(v)
                else:
                    first_hop(v)
        elif kind == "2":
            wait(st_a.at[pl.ds(FIRST.index(G[which][0]), len(G[which]))], r_a.at[GROUP[G[which][0]]])
            for v in G[which]:
                second_hop(v)
        elif kind == "3":
            wait(st_b.at[pl.ds(FIRST.index(G[which][0]), len(G[which]))], r_b.at[GROUP_B[G[which][0]]])
            for v in G[which]:
                third_hop(v)
        elif kind == "C":
            send(w_ref.at[:, columns(chip(pos) * 2 + 1 - core, 1)], mine, s_w.at[2], r_k.at[0], dev(pos, 1 - core))
        else:
            half = hbuf.at[pl.ds(pl.multiple_of(core * 512, 512), 512)]
            send(half, half, s_h, r_x, dev(pos, 1 - core))

    wait(hbuf.at[pl.ds(0, 512)], r_x)

    def product(dz, dy, first):
        wait(wbuf.at[pl.ds(0, 256)], r_k.at[dz * 4 + dy])
        k0 = pl.multiple_of((((pos[Z] - dz) % 4) * 4 + (pos[Y] - dy) % 4) * 256, 256)
        for t in range(4):
            cols = pl.ds(t * 256, 256)
            part = jnp.dot(hbuf[:, pl.ds(k0, 256)], wbuf[pl.ds(k0, 256), cols], preferred_element_type=jnp.float32)
            if first:
                acc[:, cols] = part
            else:
                acc[:, cols] += part

    for n, line in enumerate(ORDER[: 16 - LATE]):
        product(*_mirror(line, core), n == 0)
    for dz, dy in [_mirror(line, core) for line in ORDER[16 - LATE :]]:
        wait(wbuf.at[pl.ds(0, 256)], r_k.at[dz * 4 + dy])

    wait(st_a, s_w.at[0])
    wait(st_b, s_w.at[1])
    wait(wbuf.at[pl.ds(0, 127 * 32)], s_w.at[2])
    wait(hbuf.at[pl.ds(0, 63 * 8 + 512)], s_h)


def _mirror(line, core):
    return tuple(d if d in (0, 2) else d + core * (4 - 2 * d) for d in line)


def _finish(acc, hbuf, wbuf, out_ref, stage, sem):
    dp = lax.axis_index("dp")
    z, y = dp // 4, dp % 4
    core = lax.axis_index('tp') % 2
    lines = [_mirror(t, core) for t in ORDER[16 - LATE :]]
    starts = [pl.multiple_of((((z - dz) % 4) * 4 + (y - dy) % 4) * 256, 256) for dz, dy in lines]
    W = 512

    def step(t):
        cols = pl.ds(t * W, W)
        val = acc[:, cols]
        for k0 in starts:
            val += jnp.dot(hbuf[:, pl.ds(k0, 256)], wbuf[pl.ds(k0, 256), cols], preferred_element_type=jnp.float32)
        for i in range(64):
            pair = jnp.concatenate([val[i * 8 : i * 8 + 8], val[512 + i * 8 : 512 + i * 8 + 8]], axis=0)
            stage[i * 16 : i * 16 + 16, cols] = pair.astype(jnp.bfloat16)
        pltpu.make_async_copy(stage.at[:, cols], out_ref.at[:, cols], sem).start()

    for t in range(1024 // W):
        step(t)
    pltpu.make_async_copy(stage, out_ref, sem).wait()


def solution(mesh):
    def local_part(hid_blk, w_blk):
        dma = pltpu.SemaphoreType.DMA
        vm = pl.BlockSpec(memory_space=pltpu.VMEM)
        acc, hbuf, wbuf = pl.pallas_call(
            _kernel,
            out_shape=[pltpu.VMEM((1024, 1024), jnp.float32), pltpu.VMEM((1024, 4096), jnp.bfloat16), pltpu.VMEM((4096, 1024), jnp.bfloat16)],
            in_specs=[pl.BlockSpec(memory_space=pl.ANY)] * 2,
            out_specs=[vm] * 3,
            scratch_shapes=[
                pltpu.VMEM((len(FIRST), 32, 2048), jnp.bfloat16),
                pltpu.VMEM((len(THREE_FLAT), 32, 2048), jnp.bfloat16),
                dma((5,)), dma((4,)), dma((16,)), dma((3,)), dma((6,)), dma, dma, dma,
            ],
            compiler_params=pltpu.CompilerParams(collective_id=0, has_side_effects=True, vmem_limit_bytes=38 * 2**20),
        )(hid_blk, w_blk)
        acc, hbuf, wbuf = (pltpu.with_memory_space_constraint(t, pltpu.VMEM) for t in (acc, hbuf, wbuf))
        return pl.pallas_call(
            _finish,
            out_shape=jax.ShapeDtypeStruct((1024, 1024), jnp.bfloat16),
            in_specs=[vm] * 3,
            out_specs=pl.BlockSpec(memory_space=pl.ANY),
            scratch_shapes=[pltpu.VMEM((1024, 1024), jnp.bfloat16), dma],
            compiler_params=pltpu.CompilerParams(vmem_limit_bytes=20 * 2**20),
        )(acc, hbuf, wbuf)

    return jax.shard_map(
        local_part,
        mesh=mesh,
        in_specs=(P(("dp", "tp"), None), P(("dp", "tp"), None)),
        out_specs=P(None, ("dp", "tp")),
        check_vma=False,
    )
```
